256 devices in a mesh: row: 4 (over z_hi, core), col: 64 (over x, y, z_lo).
Axes of the slice: x: 4, y: 4, z: 8 (z_hi: 2, z_lo: 4; z = z_hi * 4 + z_lo), core: 2. Of those that a mesh axis runs over, the one named last changes fastest.
Arguments:
- pre_act: bfloat16 [24576, 4096], P('col'), may hold values from -16 to 16
- grad_out: bfloat16 [24576, 4096], P('col', 'row'), may hold values from -6 to 6
- w_down: bfloat16 [4096, 4096], P('col', 'row'), may hold values from -0.09375 to 0.09375
Outputs:
- w_grad: float32 [4096, 4096], P('col', 'row')
- grad_pre: bfloat16 [24576, 4096], P('col', 'row')
The draws below stay inside these ranges and needn't reach their ends.
All inputs are finite; a program needn't handle non-finite values.
Results may differ from the reference program's by a relative error of at most 0.0095.
Values may be sent and summed in bfloat16 or wider, within the bound.
A program may use at most 128 MiB of HBM per device.

```python
import jax
import jax.numpy as jnp
from jax import lax

D = 4096
FF = 4096
TOKENS = 24576
N_ROW = 4


def raised(values, key, source, target, shards_of, factor):
    owner, partner = [(jnp.arange(values.shape[axis_at]) // (values.shape[axis_at] // shards_of)).reshape([-1 if axis == axis_at else 1 for axis in range(values.ndim)]) for axis_at in (source, target)]
    chosen = jax.random.permutation(key, shards_of)[partner]
    strong = (owner == chosen) | (owner == (partner + shards_of // 2) % shards_of)
    return jnp.where(strong, factor * values, values)


def block_scale(own_key, extent, split, low, largest):
    gain, own = 1.0, jax.random.fold_in(own_key, 6)
    for dim, shards_of in split:
        steps = jnp.exp(jax.random.uniform(jax.random.fold_in(own, dim), (shards_of,), jnp.float32, low / len(split), largest / len(split)))
        gain = gain * jnp.repeat(steps, extent[dim] // shards_of).reshape([-1 if axis == dim else 1 for axis in range(len(extent))])
    return gain


def scatter_about(stream_key, extent, scale, limit, cuts=(), kind=jnp.bfloat16):
    result = jax.random.normal(stream_key, extent, jnp.float32) * scale
    if len(cuts) > 0:
        result = block_scale(stream_key, extent, cuts, -0.22, 0.18) * result
    return jnp.clip(result, min=-limit, max=limit).astype(kind)


def gaussian_with(key, dims, width, most, split, heavy, kind=jnp.bfloat16):
    values = width * jax.random.normal(key, dims, jnp.float32)
    if split:
        values = values * block_scale(key, dims, split, -0.22, 0.18)
    return jnp.clip(raised(values, jax.random.fold_in(key, 3), *heavy), -most, most).astype(kind)


def setup_inputs(seed: int = 0) -> dict:
    arg_keys = jax.random.split(jax.random.key(seed), 4)
    pre_act = gaussian_with(arg_keys[0], (TOKENS, FF), 1.0, 16.0, ((0, 64),), (0, 1, 64, 4.0))
    grad_out = scatter_about(arg_keys[1], (TOKENS, D), 1.0, 6.0, ((0, 64), (1, 4)))
    w_down = scatter_about(arg_keys[2], (FF, D), FF ** -0.5, 0.09375, ((0, 64), (1, 4)))
    return dict(pre_act=pre_act, grad_out=grad_out, w_down=w_down)


def reference(pre_act, grad_out, w_down):
    hidden = jnp.maximum(pre_act, jnp.zeros((), jnp.bfloat16)).astype(jnp.bfloat16)
    scale = 1.0 / jnp.sqrt(jnp.float32(TOKENS))
    product = lax.dot_general(hidden, grad_out, (((0,), (0,)), ((), ())), preferred_element_type=jnp.float32)
    w_grad = product * scale
    block = D // N_ROW
    total = jnp.zeros((pre_act.shape[0], FF), jnp.float32)
    for quarter in range(N_ROW):
        left = grad_out[:, quarter * block:(quarter + 1) * block]
        right = w_down[:, quarter * block:(quarter + 1) * block]
        partial_sum = lax.dot_general(left, right, (((1,), (1,)), ((), ())), preferred_element_type=jnp.float32)
        rounded = lax.optimization_barrier(partial_sum.astype(jnp.bfloat16))
        total = total + rounded.astype(jnp.float32)
    grad_pre = jnp.where(pre_act > 0, total, jnp.zeros((), jnp.float32)).astype(jnp.bfloat16)
    return (w_grad, grad_pre)
```

```python
import jax
import jax.numpy as jnp
from jax import lax
from jax.experimental import pallas as pl
from jax.experimental.pallas import tpu as pltpu
from jax.sharding import Mesh
from jax.sharding import PartitionSpec as P

AXES = ("zh", "cc", "x", "y", "zl")
COL = ("x", "y", "zl")
ROW = ("zh", "cc")
MESH = pl.DeviceIdType.MESH
BF = jnp.bfloat16
F32 = jnp.float32


def body(
    pre, go, wd, wout, gout,
    a_all, p_all, w_all, pt, acc, o_keep, o_give, o_take, keep, c_give, c_take, c_send, c_in, z_in,
    g_send, g_recv, g_sum, gz_send, gz_recv,
    wz_s, wz_r, wy_s, wy_r, a_s, a_r, p_s, p_r, q_s, q_r, d_s, d_r, c_s, c_r,
    z_s, z_r, g_s, g_r, h_s, h_r,
):
    zh, cc, x, y, zl = [lax.axis_index(name) for name in AXES]
    t, q = go.shape
    half = t // 2
    u = wd.shape[0]
    v = 4 * u
    scale = 1.0 / jnp.sqrt(jnp.float32(t * 64))

    def dev(dx=0, dy=0, dz=0, core=None, other=False):
        return (
            1 - zh if other else zh,
            cc if core is None else core,
            lax.rem(x + dx, 4),
            lax.rem(y + dy, 4),
            lax.rem(zl + dz, 4),
        )

    def copy(src, dst, ss, rs, to):
        return pltpu.make_async_remote_copy(
            src_ref=src, dst_ref=dst, send_sem=ss, recv_sem=rs, device_id=to, device_id_type=MESH
        )

    twin = 1 - cc
    lead = lax.rem(x, 2)
    peers = [dev(core=twin), dev(other=True)]
    peers += [dev(dx=d, core=c) for d in (1, 2, 3) for c in (cc, twin)]
    peers += [dev(dy=d) for d in (1, 2, 3)] + [dev(dz=d) for d in (1, 2, 3)]
    barrier = pltpu.get_barrier_semaphore()
    for peer in peers:
        pl.semaphore_signal(barrier, inc=1, device_id=peer, device_id_type=MESH)
    pl.semaphore_wait(barrier, len(peers))

    sent = []

    def send(c):
        c.start()
        sent.append(c)

    def w_rows(yy, zz):
        return pl.ds(pl.multiple_of(v * yy + u * zz, u), u)

    here = w_rows(y, zl)
    for d in (1, 2, 3):
        send(copy(wd, w_all.at[here], wz_s.at[d - 1], wz_r.at[d - 1], dev(dz=d)))
    for d in (1, 2, 3):
        send(copy(wd, w_all.at[here], wy_s.at[d - 1, 0], wy_r.at[d - 1, 0], dev(dy=d)))

    def a_half(slot, h):
        return a_all.at[pl.ds(t * slot + half * h, half)]

    for h in (0, 1):
        send(copy(go.at[pl.ds(half * h, half)], a_half(1, h), a_s.at[0, h], a_r.at[0, h], dev(dx=1)))
        g = 1 - h
        send(copy(go.at[pl.ds(half * g, half)], a_half(2, g), a_s.at[1, g], a_r.at[1, g], dev(dx=3)))

    a_all[0:t] = go[...]
    w_all[here] = wd[...]

    def p_cols(dx, k):
        block = q * lax.rem(x + dx, 4) + v * lax.rem(y + 1 + k, 4)
        return pl.ds(pl.multiple_of(block, v), v)

    for k in range(4):
        p_all[k, 0:t] = pre[:, p_cols(0, k)]

    for d in (1, 2, 3):
        rows = w_rows(y, lax.rem(zl + 4 - d, 4))
        copy(wd, w_all.at[rows], wz_s.at[d - 1], wz_r.at[d - 1], dev(dz=d)).wait_recv()
        for e in (1, 2, 3):
            send(copy(w_all.at[rows], w_all.at[rows], wy_s.at[e - 1, d], wy_r.at[e - 1, d], dev(dy=e)))

    def a_wait(slot, h):
        copy(a_half(slot, h), a_half(slot, h), a_s.at[slot - 1, h], a_r.at[slot - 1, h], dev(dx=1)).wait_recv()

    a_wait(1, 0)
    send(copy(a_half(1, 0), a_half(3, 0), a_s.at[2, 0], a_r.at[2, 0], dev(dx=1)))
    a_wait(2, 1)
    send(copy(a_half(2, 1), a_half(3, 1), a_s.at[2, 1], a_r.at[2, 1], dev(dx=3)))

    for e in (1, 2, 3):
        for d in range(4):
            rows = w_rows(lax.rem(y + 4 - e, 4), lax.rem(zl + 4 - d, 4))
            copy(wd, w_all.at[rows], wy_s.at[e - 1, d], wy_r.at[e - 1, d], dev(dy=e)).wait_recv()

    mine = pl.ds(pl.multiple_of(half * cc, half), half)
    theirs = pl.ds(pl.multiple_of(half * twin, half), half)

    def partial(slot, out):
        @pl.loop(0, 4)
        def _(n):
            cols = pl.ds(pl.multiple_of(n * v, v), v)
            out[:, cols] = lax.dot_general(
                a_all[t * slot:t * slot + t], w_all[cols, :], (((1,), (1,)), ((), ())),
                preferred_element_type=F32,
            )

    def swap(slot):
        return copy(c_give.at[slot - 1], c_take.at[slot - 1], d_s.at[slot], d_r.at[slot], dev(core=twin))

    def offer(slot):
        partial(slot, acc)
        c_give[slot - 1] = acc[theirs].astype(BF)
        keep[slot - 1] = acc[mine]
        send(swap(slot))

    def deliver(slot, dx):
        swap(slot).wait_recv()
        c_send[slot - 1] = (keep[slot - 1] + c_take[slot - 1].astype(F32)).astype(BF)
        target = c_in.at[lax.div(x, 2), mine]
        send(copy(c_send.at[slot - 1], target, c_s.at[slot - 1], c_r.at[lax.div(x, 2), cc], dev(dx=dx, core=lead)))

    def arrived(i, h):
        rows = c_in.at[i, pl.ds(half * h, half)]
        copy(rows, rows, c_s.at[0], c_r.at[i, h], dev(dx=1)).wait_recv()

    def across(h):
        rows = pl.ds(half * h, half)
        return copy(c_in.at[1 - zh, rows], z_in.at[rows], z_s.at[h], z_r.at[h], dev(other=True))

    far = lax.rem(2 * (1 - zh) + cc + 4 - x, 4)

    def onward():
        for h in (0, 1):
            arrived(1 - zh, h)
            across(h).start()

    partial(0, o_keep)
    own = copy(o_give, o_take, d_s.at[0], d_r.at[0], dev(core=twin))

    @pl.when(cc != lead)
    def _():
        o_give[...] = o_keep[...].astype(BF)
        own.start()

    a_wait(1, 1)
    offer(1)

    @pl.when(cc == lead)
    def _():
        own.wait_recv()
        c_in[lax.div(x, 2)] = (o_keep[...] + o_take[...].astype(F32)).astype(BF)

        @pl.when(far == 0)
        def _():
            for h in (0, 1):
                across(h).start()

    a_wait(2, 0)
    offer(2)
    deliver(1, 3)
    deliver(2, 1)
    a_wait(3, 0)
    a_wait(3, 1)
    offer(3)

    def p_copy(slot, k):
        dx = (1, 3, 2)[slot - 1]
        rows = pl.ds(pl.multiple_of(t * slot + half * cc, half), half)
        return copy(
            pre.at[mine, p_cols(dx, k)], p_all.at[k, rows], p_s.at[slot - 1, k], p_r.at[slot - 1, k], dev(dx=dx)
        )

    def q_copy(slot, k):
        rows = p_all.at[k, pl.ds(pl.multiple_of(t * slot + half * cc, half), half)]
        return copy(rows, rows, q_s.at[slot - 1, k], q_r.at[slot - 1, k], dev(core=twin))

    for k in range(4):
        for slot in (1, 2, 3):
            send(p_copy(slot, k))
    deliver(3, 2)

    @pl.when((far == 1) | (far == 3))
    def _():
        onward()

    def g_copy(k):
        return copy(g_send.at[k], g_recv.at[k], g_s.at[k], g_r.at[k], dev(dy=1 + k))

    for k in range(4):
        for slot in (1, 2, 3):
            p_copy(slot, k).wait_recv()
            send(q_copy(slot, k))
        for slot in (1, 2, 3):
            q_copy(slot, k).wait_recv()
        pt[...] = jnp.maximum(p_all[k], jnp.zeros((), BF)).T

        @pl.loop(0, 4)
        def _(n):
            cols = pl.ds(pl.multiple_of(n * v, v), v)
            part = jnp.dot(pt[...], a_all[:, cols], preferred_element_type=F32)
            if k < 3:
                g_send[k, :, cols] = part.astype(BF)
            else:
                g_sum[:, cols] = part

        if k < 3:
            send(g_copy(k))

    @pl.when(far == 2)
    def _():
        onward()

    for k in range(3):
        g_copy(k).wait_recv()
    g_sum[...] += g_recv[0].astype(F32) + g_recv[1].astype(F32) + g_recv[2].astype(F32)

    def h_copy(d):
        return copy(gz_send.at[d - 1], gz_recv.at[d - 1], h_s.at[d - 1], h_r.at[d - 1], dev(dz=d))

    for d in (1, 2, 3):
        gz_send[d - 1] = g_sum[pl.ds(pl.multiple_of(u * lax.rem(zl + d, 4), u), u)].astype(BF)
        send(h_copy(d))
    for d in (1, 2, 3):
        h_copy(d).wait_recv()
    total = g_sum[pl.ds(pl.multiple_of(u * zl, u), u)]
    total += gz_recv[0].astype(F32) + gz_recv[1].astype(F32) + gz_recv[2].astype(F32)
    wout[...] = total * scale

    @pl.when(x != 2 * zh + cc)
    def _():
        for h in (0, 1):
            arrived(zh, h)

    for h in (0, 1):
        across(h).wait_recv()
    own_pre = pre[:, pl.ds(pl.multiple_of(q * (2 * zh + cc), q), q)]
    both = c_in[zh].astype(F32) + z_in[...].astype(F32)
    gout[...] = jnp.where(own_pre.astype(F32) > 0, both, 0.0).astype(BF)

    for c in sent:
        c.wait_send()
    for h in (0, 1):
        across(h).wait_send()

    @pl.when(cc != lead)
    def _():
        own.wait_send()


def per_device(pre_act, grad_out, w_down):
    t, q = grad_out.shape
    u = w_down.shape[0]
    v = 4 * u
    half = t // 2
    vm = pltpu.VMEM
    sem = lambda *n: pltpu.SemaphoreType.DMA(n)
    space = pl.BlockSpec(memory_space=pltpu.VMEM)
    return pl.pallas_call(
        body,
        out_shape=(jax.ShapeDtypeStruct((u, q), F32), jax.ShapeDtypeStruct((t, q), BF)),
        in_specs=[space] * 3,
        out_specs=(space, space),
        scratch_shapes=[
            vm((4 * t, q), BF), vm((4, 4 * t, v), BF), vm((4 * v, q), BF), vm((v, 4 * t), BF),
            vm((t, q), F32), vm((t, q), F32), vm((t, q), BF), vm((t, q), BF),
            vm((3, half, q), F32), vm((3, half, q), BF), vm((3, half, q), BF), vm((3, half, q), BF),
            vm((2, t, q), BF), vm((t, q), BF),
            vm((3, v, q), BF), vm((3, v, q), BF), vm((v, q), F32), vm((3, u, q), BF), vm((3, u, q), BF),
            sem(3), sem(3), sem(3, 4), sem(3, 4), sem(3, 2), sem(3, 2), sem(3, 4), sem(3, 4), sem(3, 4), sem(3, 4),
            sem(4), sem(4), sem(3), sem(2, 2),
            sem(2), sem(2), sem(3), sem(3), sem(3), sem(3),
        ],
        compiler_params=pltpu.CompilerParams(
            collective_id=0, has_side_effects=True, vmem_limit_bytes=60 * 2**20
        ),
        name="backward",
    )(pre_act, grad_out, w_down)


def solution(mesh):
    torus = Mesh(mesh.devices.reshape(2, mesh.shape["row"] // 2, 4, 4, 4), AXES)
    return jax.shard_map(
        per_device,
        mesh=torus,
        in_specs=(P(COL, None), P(COL, ROW), P(COL, ROW)),
        out_specs=(P(COL, ROW), P(COL, ROW)),
        check_vma=False,
    )
```

```python
import jax
import jax.numpy as jnp
from jax import lax
from jax.experimental import pallas as pl
from jax.experimental.pallas import tpu as pltpu
from jax.sharding import Mesh
from jax.sharding import PartitionSpec as P

AXES = ("zh", "cc", "x", "y", "zl")
COL = ("x", "y", "zl")
ROW = ("zh", "cc")
MESH = pl.DeviceIdType.MESH
BF = jnp.bfloat16
F32 = jnp.float32
TURNS = (1, 3, 2, 0)
FROM = (0, 1, 3, 2)


def body(
    pre_h, go_h, wd_h, wout, gout,
    pre, a_all, p_all, w_all, pt, acc, o_keep, o_give, o_take, keep, c_give, c_take, c_send, c_in, z_in,
    g_send, g_recv, g_sum, gz_send, gz_recv,
    l_s, wz_s, wz_r, wy_s, wy_r, a_s, a_r, p_s, p_r, q_s, q_r, o_s, o_r, d_s, d_r, c_s, c_r,
    z_s, z_r, g_s, g_r, h_s, h_r,
):
    zh, cc, x, y, zl = [lax.axis_index(name) for name in AXES]
    t, q = go_h.shape
    half = t // 2
    u = wd_h.shape[0]
    v = 4 * u
    scale = 1.0 / jnp.sqrt(jnp.float32(t * 64))

    def dev(dx=0, dy=0, dz=0, core=None, other=False):
        return (
            1 - zh if other else zh,
            cc if core is None else core,
            lax.rem(x + dx, 4),
            lax.rem(y + dy, 4),
            lax.rem(zl + dz, 4),
        )

    def copy(src, dst, ss, rs, to):
        return pltpu.make_async_remote_copy(
            src_ref=src, dst_ref=dst, send_sem=ss, recv_sem=rs, device_id=to, device_id_type=MESH
        )

    def w_rows(yy, zz):
        return pl.ds(pl.multiple_of(v * yy + u * zz, u), u)

    def w_block(dy, d):
        return w_all.at[w_rows(lax.rem(y + 4 - dy, 4), lax.rem(zl + 4 - d, 4))]

    def p_cols(dx, k):
        block = q * lax.rem(x + dx, 4) + v * lax.rem(y + TURNS[k], 4)
        return pl.ds(pl.multiple_of(block, v), v)

    twin = 1 - cc
    lead = lax.rem(x, 2)
    peers = [dev(core=twin), dev(other=True)]
    peers += [dev(dx=d, core=c) for d in (1, 2, 3) for c in (cc, twin)]
    peers += [dev(dy=d) for d in (1, 2, 3)] + [dev(dz=d) for d in (1, 2, 3)]
    with jax.named_scope("s00_barrier"):
        barrier = pltpu.get_barrier_semaphore()
        for peer in peers:
            pl.semaphore_signal(barrier, inc=1, device_id=peer, device_id_type=MESH)

    load_w = pltpu.make_async_copy(wd_h, w_block(0, 0), l_s.at[0])
    load_a = pltpu.make_async_copy(go_h, a_all.at[0:t], l_s.at[1])
    load_p = pltpu.make_async_copy(pre_h, pre, l_s.at[2])
    loads = [load_w, load_a, load_p]
    for c in loads:
        c.start()
    with jax.named_scope("s01_loads"):
        load_w.wait()
        load_a.wait()
    with jax.named_scope("s02_barrier"):
        pl.semaphore_wait(barrier, len(peers))

    sent = []

    def send(c):
        c.start()
        sent.append(c)

    def wz(d):
        return copy(w_block(0, 0), w_block(0, 0), wz_s.at[d - 1], wz_r.at[d - 1], dev(dz=d))

    def wy(e, d):
        block = (w_block(0, d), w_block(0, d), w_block(1, d) if d % 2 == 0 else w_block(3, d))[e]
        dy = (1, 3, 1 if d % 2 == 0 else 3)[e]
        return copy(block, block, wy_s.at[e, d], wy_r.at[e, d], dev(dy=dy))

    def wy_wait(e, d):
        block = w_block((1, 3, 2)[e], d)
        copy(block, block, wy_s.at[e, d], wy_r.at[e, d], dev(dy=1)).wait_recv()

    def a_half(slot, h):
        return a_all.at[pl.ds(t * slot + half * h, half)]

    for d in (1, 2, 3):
        send(wz(d))
    send(wy(0, 0))
    send(wy(1, 0))
    for h in (0, 1):
        send(copy(a_half(0, h), a_half(1, h), a_s.at[0, h], a_r.at[0, h], dev(dx=1)))
        g = 1 - h
        send(copy(a_half(0, g), a_half(2, g), a_s.at[1, g], a_r.at[1, g], dev(dx=3)))

    mine = pl.ds(pl.multiple_of(half * cc, half), half)
    theirs = pl.ds(pl.multiple_of(half * twin, half), half)

    def p_copy(slot, k):
        dx = (1, 3, 2)[slot - 1]
        rows = pl.ds(pl.multiple_of(t * slot + half * cc, half), half)
        return copy(
            pre.at[mine, p_cols(dx, k)], p_all.at[k, rows], p_s.at[slot - 1, k], p_r.at[slot - 1, k], dev(dx=dx)
        )

    def q_copy(slot, k):
        rows = p_all.at[k, pl.ds(pl.multiple_of(t * slot + half * cc, half), half)]
        return copy(rows, rows, q_s.at[slot - 1, k], q_r.at[slot - 1, k], dev(core=twin))

    def p_send(k):
        for slot in (1, 2, 3):
            send(p_copy(slot, k))

    load_p.wait()
    p_send(0)

    with jax.named_scope("s03_local"):
        for k in range(4):
            p_all[k, 0:t] = pre[:, p_cols(0, k)]

    def a_wait(slot, h):
        copy(a_half(slot, h), a_half(slot, h), a_s.at[slot - 1, h], a_r.at[slot - 1, h], dev(dx=1)).wait_recv()

    def a_relay():
        a_wait(1, 0)
        send(copy(a_half(1, 0), a_half(3, 0), a_s.at[2, 0], a_r.at[2, 0], dev(dx=1)))
        a_wait(2, 1)
        send(copy(a_half(2, 1), a_half(3, 1), a_s.at[2, 1], a_r.at[2, 1], dev(dx=3)))

    for d in (1, 2, 3):
        with jax.named_scope("s04_wz"):
            block = w_block(0, d)
            copy(block, block, wz_s.at[d - 1], wz_r.at[d - 1], dev(dz=d)).wait_recv()
            send(wy(0, d))
            send(wy(1, d))
        with jax.named_scope("s05_wy"):
            wy_wait((d - 1) % 2, d - 1)
            send(wy(2, d - 1))
        if d == 2:
            with jax.named_scope("s05_arelay"):
                a_relay()
    with jax.named_scope("s05_wy"):
        wy_wait(1, 3)
        send(wy(2, 3))

    def w_cols(n):
        return pl.ds(pl.multiple_of(v * lax.rem(y + 4 - FROM[n], 4), v), v)

    def partial(slot, n, out):
        out[...] = lax.dot_general(
            a_all[t * slot:t * slot + t], w_all[w_cols(n), :], (((1,), (1,)), ((), ())),
            preferred_element_type=F32,
        )

    def swap(slot, n):
        i = slot - 1
        return copy(c_give.at[i, n], c_take.at[i, n], d_s.at[i, n], d_r.at[i, n], dev(core=twin))

    def offer(slot, n):
        partial(slot, n, acc)
        c_give[slot - 1, n] = acc[theirs].astype(BF)
        keep[slot - 1, n] = acc[mine]
        send(swap(slot, n))

    def deliver(slot, n):
        i = slot - 1
        swap(slot, n).wait_recv()
        c_send[i, n] = (keep[i, n] + c_take[i, n].astype(F32)).astype(BF)
        target = c_in.at[lax.div(x, 2), n, mine]
        to = dev(dx=(3, 1, 2)[i], core=lead)
        send(copy(c_send.at[i, n], target, c_s.at[i, n], c_r.at[lax.div(x, 2), n, cc], to))

    def arrived(i, n):
        for h in (0, 1):
            rows = c_in.at[i, n, pl.ds(half * h, half)]
            copy(rows, rows, c_s.at[0, 0], c_r.at[i, n, h], dev(dx=1)).wait_recv()

    def across(n):
        return copy(c_in.at[1 - zh, n], z_in.at[n], z_s.at[n], z_r.at[n], dev(other=True))

    far = lax.rem(2 * (1 - zh) + cc + 4 - x, 4)

    def onward():
        for n in range(4):
            arrived(1 - zh, n)
            across(n).start()

    with jax.named_scope("s06_a12"):
        a_wait(1, 1)
        a_wait(2, 0)
    for n in range(4):
        with jax.named_scope("s07_wy"):
            if n in (1, 2):
                for d in range(4):
                    if d % 2 == n % 2:
                        wy_wait(n - 1, d)
            if n == 3:
                for d in range(4):
                    wy_wait(2, d)
        with jax.named_scope("s08_offer12"):
            offer(1, n)
            offer(2, n)
            if n > 0:
                deliver(1, n - 1)
                deliver(2, n - 1)
    with jax.named_scope("s08_deliver12"):
        deliver(1, 3)
        deliver(2, 3)

    own = copy(o_give, o_take, o_s.at[0], o_r.at[0], dev(core=twin))
    with jax.named_scope("s09_own"):
        for n in range(4):
            partial(0, n, o_keep.at[n])

        @pl.when(cc != lead)
        def _():
            o_give[...] = o_keep[...].astype(BF)
            own.start()

    with jax.named_scope("s10_a3"):
        a_wait(3, 0)
        a_wait(3, 1)
    with jax.named_scope("s10_offer3"):
        for n in range(4):
            offer(3, n)

    with jax.named_scope("s11_own"):

        @pl.when(cc == lead)
        def _():
            own.wait_recv()
            c_in[lax.div(x, 2)] = (o_keep[...] + o_take[...].astype(F32)).astype(BF)

            @pl.when(far == 0)
            def _():
                for n in range(4):
                    across(n).start()

    def onward3(n):
        @pl.when(far == 2)
        def _():
            arrived(1 - zh, n)
            across(n).start()

    with jax.named_scope("s12_deliver3"):
        p_send(1)
        deliver(3, 0)
        p_send(2)
        deliver(3, 1)
        deliver(3, 2)
        p_send(3)
        deliver(3, 3)

    with jax.named_scope("s13_onward1"):

        @pl.when((far == 1) | (far == 3))
        def _():
            onward()

    def g_copy(k, w):
        return copy(g_send.at[k, w], g_recv.at[k, w], g_s.at[k, w], g_r.at[k, w], dev(dy=TURNS[k]))

    def weight_part(k):
        with jax.named_scope("s14_pwait"):
            for slot in (1, 2, 3):
                p_copy(slot, k).wait_recv()
                send(q_copy(slot, k))
        with jax.named_scope("s15_qwait"):
            for slot in (1, 2, 3):
                q_copy(slot, k).wait_recv()
        with jax.named_scope("s16_g"):
            pt[...] = jnp.maximum(p_all[k], jnp.zeros((), BF)).T

            for w in (0, 1):

                @pl.loop(0, 2)
                def _(n):
                    cols = pl.ds(pl.multiple_of(n * v, v), v)
                    from_cols = pl.ds(pl.multiple_of((2 * w + n) * v, v), v)
                    part = jnp.dot(pt[...], a_all[:, from_cols], preferred_element_type=F32)
                    if k < 3:
                        g_send[k, w, :, cols] = part.astype(BF)
                    else:
                        g_sum[w, :, cols] = part

                if k < 3:
                    send(g_copy(k, w))

    weight_part(0)
    weight_part(1)
    with jax.named_scope("s17_onward3"):
        onward3(0)
    weight_part(2)
    with jax.named_scope("s17_onward3"):
        onward3(1)
        onward3(2)
    weight_part(3)

    def h_copy(w, d):
        return copy(gz_send.at[w, d - 1], gz_recv.at[w, d - 1], h_s.at[w, d - 1], h_r.at[w, d - 1], dev(dz=d))

    def over_y(w):
        with jax.named_scope("s20_gwait"):
            for k in range(3):
                g_copy(k, w).wait_recv()
        g_sum[w] += g_recv[0, w].astype(F32) + g_recv[1, w].astype(F32) + g_recv[2, w].astype(F32)
        for d in (1, 2, 3):
            gz_send[w, d - 1] = g_sum[w, pl.ds(pl.multiple_of(u * lax.rem(zl + d, 4), u), u)].astype(BF)
            send(h_copy(w, d))

    over_y(0)
    with jax.named_scope("s17_onward3"):
        onward3(3)
    over_y(1)

    with jax.named_scope("s21_cwait"):

        @pl.when(x != 2 * zh + cc)
        def _():
            for n in range(4):
                arrived(zh, n)

    with jax.named_scope("s22_zwait"):
        for n in range(4):
            across(n).wait_recv()
    for n in range(4):
        cols = w_cols(n)
        own_pre = pre[:, pl.ds(pl.multiple_of(q * (2 * zh + cc) + v * lax.rem(y + 4 - FROM[n], 4), v), v)]
        both = c_in[zh, n].astype(F32) + z_in[n].astype(F32)
        gout[:, cols] = jnp.where(own_pre.astype(F32) > 0, both, 0.0).astype(BF)

    for w in (0, 1):
        with jax.named_scope("s23_hwait"):
            for d in (1, 2, 3):
                h_copy(w, d).wait_recv()
        total = g_sum[w, pl.ds(pl.multiple_of(u * zl, u), u)]
        total += gz_recv[w, 0].astype(F32) + gz_recv[w, 1].astype(F32) + gz_recv[w, 2].astype(F32)
        wout[:, w * 2 * v:(w + 1) * 2 * v] = total * scale

    for c in sent:
        c.wait_send()
    for n in range(4):
        across(n).wait_send()

    @pl.when(cc != lead)
    def _():
        own.wait_send()


def per_device(pre_act, grad_out, w_down):
    t, q = grad_out.shape
    u = w_down.shape[0]
    v = 4 * u
    half = t // 2
    vm = pltpu.VMEM
    sem = lambda *n: pltpu.SemaphoreType.DMA(n)
    space = pl.BlockSpec(memory_space=pltpu.VMEM)
    hbm = pl.BlockSpec(memory_space=pltpu.HBM)
    outs = pl.pallas_call(
        body,
        out_shape=(pltpu.VMEM((u, q), F32), pltpu.VMEM((t, q), BF)),
        in_specs=[hbm] * 3,
        out_specs=(space, space),
        scratch_shapes=[
            vm((t, pre_act.shape[1]), BF),
            vm((4 * t, q), BF), vm((4, 4 * t, v), BF), vm((4 * v, q), BF), vm((v, 4 * t), BF),
            vm((t, v), F32), vm((4, t, v), F32), vm((4, t, v), BF), vm((4, t, v), BF),
            vm((3, 4, half, v), F32), vm((3, 4, half, v), BF), vm((3, 4, half, v), BF), vm((3, 4, half, v), BF),
            vm((2, 4, t, v), BF), vm((4, t, v), BF),
            vm((3, 2, v, q // 2), BF), vm((3, 2, v, q // 2), BF), vm((2, v, q // 2), F32),
            vm((2, 3, u, q // 2), BF), vm((2, 3, u, q // 2), BF),
            sem(3), sem(3), sem(3), sem(3, 4), sem(3, 4), sem(3, 2), sem(3, 2),
            sem(3, 4), sem(3, 4), sem(3, 4), sem(3, 4),
            sem(1), sem(1), sem(3, 4), sem(3, 4), sem(3, 4), sem(2, 4, 2),
            sem(4), sem(4), sem(3, 2), sem(3, 2), sem(2, 3), sem(2, 3),
        ],
        compiler_params=pltpu.CompilerParams(
            collective_id=0, has_side_effects=True, vmem_limit_bytes=62_400_000
        ),
        name="backward",
    )(pre_act, grad_out, w_down)
    return outs[0], outs[1]


def solution(mesh):
    torus = Mesh(mesh.devices.reshape(2, mesh.shape["row"] // 2, 4, 4, 4), AXES)
    return jax.shard_map(
        per_device,
        mesh=torus,
        in_specs=(P(COL, None), P(COL, ROW), P(COL, ROW)),
        out_specs=(P(COL, ROW), P(COL, ROW)),
        check_vma=False,
    )
```

```python
import jax
import jax.numpy as jnp
from jax import lax
from jax.experimental import pallas as pl
from jax.experimental.pallas import tpu as pltpu
from jax.sharding import Mesh
from jax.sharding import PartitionSpec as P

AXES = ("zh", "cc", "x", "y", "zl")
COL = ("x", "y", "zl")
ROW = ("zh", "cc")
MESH = pl.DeviceIdType.MESH
BF = jnp.bfloat16
F32 = jnp.float32
TURNS = (2, 1, 3, 0)
PLAN = (
    "p0", "z1", "w0", "z2", "w1", "z3", "b1", "b2", "c0", "w2", "w3", "c1",
    "e0", "c2", "e1", "ar", "c3", "e2", "e3", "p1", "ow", "n0", "n1", "of",
    "q0", "a3", "g0", "n2", "n3", "o0", "o1", "d0", "o2", "d1", "p2", "o3",
    "d2", "p3", "d3", "q1", "g1", "r0", "r1", "q2", "g2", "r2", "q3", "g3",
    "r3", "y0", "y1",
)
FROM = (0, 1, 3, 2)


def body(
    pre_h, go_h, wd_h, wout, gout,
    pre, a_all, p_all, w_all, pt, acc, o_keep, o_give, o_take, keep, c_give, c_take, c_send, c_in, z_in,
    g_send, g_recv, g_sum, gz_send, gz_recv,
    l_s, wz_s, wz_r, wy_s, wy_r, a_s, a_r, p_s, p_r, q_s, q_r, o_s, o_r, d_s, d_r, c_s, c_r,
    z_s, z_r, g_s, g_r, h_s, h_r,
):
    zh, cc, x, y, zl = [lax.axis_index(name) for name in AXES]
    t, q = go_h.shape
    half = t // 2
    u = wd_h.shape[0]
    v = 4 * u
    scale = 1.0 / jnp.sqrt(jnp.float32(t * 64))

    def dev(dx=0, dy=0, dz=0, core=None, other=False):
        return (
            1 - zh if other else zh,
            cc if core is None else core,
            lax.rem(x + dx, 4),
            lax.rem(y + dy, 4),
            lax.rem(zl + dz, 4),
        )

    def copy(src, dst, ss, rs, to):
        return pltpu.make_async_remote_copy(
            src_ref=src, dst_ref=dst, send_sem=ss, recv_sem=rs, device_id=to, device_id_type=MESH
        )

    def w_rows(yy, zz):
        return pl.ds(pl.multiple_of(v * yy + u * zz, u), u)

    def w_block(dy, d):
        return w_all.at[w_rows(lax.rem(y + 4 - dy, 4), lax.rem(zl + 4 - d, 4))]

    def p_cols(dx, k):
        block = q * lax.rem(x + dx, 4) + v * lax.rem(y + TURNS[k], 4)
        return pl.ds(pl.multiple_of(block, v), v)

    twin = 1 - cc
    lead = lax.rem(x, 2)
    peers = [dev(core=twin), dev(other=True)]
    peers += [dev(dx=d, core=c) for d in (1, 2, 3) for c in (cc, twin)]
    peers += [dev(dy=d) for d in (1, 2, 3)] + [dev(dz=d) for d in (1, 2, 3)]
    with jax.named_scope("s00_barrier"):
        barrier = pltpu.get_barrier_semaphore()
        for peer in peers:
            pl.semaphore_signal(barrier, inc=1, device_id=peer, device_id_type=MESH)

    load_w = pltpu.make_async_copy(wd_h, w_block(0, 0), l_s.at[0])
    load_a = pltpu.make_async_copy(go_h, a_all.at[0:t], l_s.at[1])
    load_p = pltpu.make_async_copy(pre_h, pre, l_s.at[2])
    loads = [load_w, load_a, load_p]
    for c in loads:
        c.start()
    with jax.named_scope("s01_loads"):
        load_w.wait()
        load_a.wait()
    with jax.named_scope("s02_barrier"):
        pl.semaphore_wait(barrier, len(peers))

    sent = []

    def send(c):
        c.start()
        sent.append(c)

    def wz(d):
        return copy(w_block(0, 0), w_block(0, 0), wz_s.at[d - 1], wz_r.at[d - 1], dev(dz=d))

    def wy(e, d):
        block = (w_block(0, d), w_block(0, d), w_block(1, d) if d % 2 == 0 else w_block(3, d))[e]
        dy = (1, 3, 1 if d % 2 == 0 else 3)[e]
        return copy(block, block, wy_s.at[e, d], wy_r.at[e, d], dev(dy=dy))

    def wy_wait(e, d):
        block = w_block((1, 3, 2)[e], d)
        copy(block, block, wy_s.at[e, d], wy_r.at[e, d], dev(dy=1)).wait_recv()

    def a_half(slot, h):
        return a_all.at[pl.ds(t * slot + half * h, half)]

    for d in (1, 2, 3):
        send(wz(d))
    send(wy(0, 0))
    send(wy(1, 0))
    for h in (0, 1):
        send(copy(a_half(0, h), a_half(1, h), a_s.at[0, h], a_r.at[0, h], dev(dx=1)))
        g = 1 - h
        send(copy(a_half(0, g), a_half(2, g), a_s.at[1, g], a_r.at[1, g], dev(dx=3)))

    mine = pl.ds(pl.multiple_of(half * cc, half), half)
    theirs = pl.ds(pl.multiple_of(half * twin, half), half)

    def p_copy(slot, k):
        dx = (1, 3, 2)[slot - 1]
        rows = pl.ds(pl.multiple_of(t * slot + half * cc, half), half)
        return copy(
            pre.at[mine, p_cols(dx, k)], p_all.at[k, rows], p_s.at[slot - 1, k], p_r.at[slot - 1, k], dev(dx=dx)
        )

    def q_copy(slot, k):
        rows = p_all.at[k, pl.ds(pl.multiple_of(t * slot + half * cc, half), half)]
        return copy(rows, rows, q_s.at[slot - 1, k], q_r.at[slot - 1, k], dev(core=twin))

    def p_send(k):
        for slot in (1, 2, 3):
            send(p_copy(slot, k))

    load_p.wait()

    with jax.named_scope("s03_local"):
        for k in range(4):
            p_all[k, 0:t] = pre[:, p_cols(0, k)]

    def a_wait(slot, h):
        copy(a_half(slot, h), a_half(slot, h), a_s.at[slot - 1, h], a_r.at[slot - 1, h], dev(dx=1)).wait_recv()

    def a_relay():
        send(copy(a_half(1, 0), a_half(3, 0), a_s.at[2, 0], a_r.at[2, 0], dev(dx=1)))
        send(copy(a_half(2, 1), a_half(3, 1), a_s.at[2, 1], a_r.at[2, 1], dev(dx=3)))

    def w_relay(d):
        with jax.named_scope("s05_wy"):
            wy_wait(d % 2, d)
            send(wy(2, d))

    def w_take(d):
        with jax.named_scope("s04_wz"):
            block = w_block(0, d)
            copy(block, block, wz_s.at[d - 1], wz_r.at[d - 1], dev(dz=d)).wait_recv()
            send(wy(0, d))
            send(wy(1, d))

    def w_cols(n):
        return pl.ds(pl.multiple_of(v * lax.rem(y + 4 - FROM[n], 4), v), v)

    def partial(slot, n, out):
        out[...] = lax.dot_general(
            a_all[t * slot:t * slot + t], w_all[w_cols(n), :], (((1,), (1,)), ((), ())),
            preferred_element_type=F32,
        )

    def swap(slot, n):
        i = slot - 1
        return copy(c_give.at[i, n], c_take.at[i, n], d_s.at[i, n], d_r.at[i, n], dev(core=twin))

    def offer(slot, n):
        partial(slot, n, acc)
        c_give[slot - 1, n] = acc[theirs].astype(BF)
        keep[slot - 1, n] = acc[mine]
        send(swap(slot, n))

    def deliver(slot, n):
        i = slot - 1
        swap(slot, n).wait_recv()
        c_send[i, n] = (keep[i, n] + c_take[i, n].astype(F32)).astype(BF)
        target = c_in.at[lax.div(x, 2), n, mine]
        to = dev(dx=(3, 1, 2)[i], core=lead)
        send(copy(c_send.at[i, n], target, c_s.at[i, n], c_r.at[lax.div(x, 2), n, cc], to))

    def arrived(i, n):
        for h in (0, 1):
            rows = c_in.at[i, n, pl.ds(half * h, half)]
            copy(rows, rows, c_s.at[0, 0], c_r.at[i, n, h], dev(dx=1)).wait_recv()

    def across(n):
        return copy(c_in.at[1 - zh, n], z_in.at[n], z_s.at[n], z_r.at[n], dev(other=True))

    far = lax.rem(2 * (1 - zh) + cc + 4 - x, 4)

    def onward(n):
        with jax.named_scope("s10_onward1"):

            @pl.when((far == 1) | (far == 3))
            def _():
                arrived(1 - zh, n)
                across(n).start()

    def near(n):
        with jax.named_scope("s07_wy"):
            if n in (1, 2):
                for d in range(4):
                    if d % 2 == n % 2:
                        wy_wait(n - 1, d)
            if n == 3:
                for d in range(4):
                    wy_wait(2, d)
        with jax.named_scope("s08_offer12"):
            offer(1, n)
            offer(2, n)

    def near_out(n):
        with jax.named_scope("s08_deliver12"):
            deliver(1, n)
            deliver(2, n)

    own = copy(o_give, o_take, o_s.at[0], o_r.at[0], dev(core=twin))

    def own_part():
        with jax.named_scope("s09_own"):
            for n in range(4):
                partial(0, n, o_keep.at[n])

            @pl.when(cc != lead)
            def _():
                o_give[...] = o_keep[...].astype(BF)
                own.start()

    def own_sum():
        with jax.named_scope("s11_own"):

            @pl.when(cc == lead)
            def _():
                own.wait_recv()
                c_in[lax.div(x, 2)] = (o_keep[...] + o_take[...].astype(F32)).astype(BF)

                @pl.when(far == 0)
                def _():
                    for n in range(4):
                        across(n).start()

    def p_pass(k):
        with jax.named_scope("s14_pwait"):
            for slot in (1, 2, 3):
                p_copy(slot, k).wait_recv()
                send(q_copy(slot, k))

    def g_copy(k, w):
        return copy(g_send.at[k, w], g_recv.at[k, w], g_s.at[k, w], g_r.at[k, w], dev(dy=TURNS[k]))

    def weight_part(k):
        with jax.named_scope("s15_qwait"):
            for slot in (1, 2, 3):
                q_copy(slot, k).wait_recv()
        with jax.named_scope("s16_g"):
            pt[...] = jnp.maximum(p_all[k], jnp.zeros((), BF)).T

            for w in (0, 1):

                @pl.loop(0, 2)
                def _(n):
                    cols = pl.ds(pl.multiple_of(n * v, v), v)
                    from_cols = pl.ds(pl.multiple_of((2 * w + n) * v, v), v)
                    part = jnp.dot(pt[...], a_all[:, from_cols], preferred_element_type=F32)
                    if k < 3:
                        g_send[k, w, :, cols] = part.astype(BF)
                    else:
                        g_sum[w, :, cols] = part

                if k < 3:
                    send(g_copy(k, w))

    def onward3(n):
        with jax.named_scope("s17_onward3"):

            @pl.when(far == 2)
            def _():
                arrived(1 - zh, n)
                across(n).start()

    def h_copy(w, d):
        return copy(gz_send.at[w, d - 1], gz_recv.at[w, d - 1], h_s.at[w, d - 1], h_r.at[w, d - 1], dev(dz=d))

    def over_y(w):
        with jax.named_scope("s20_gwait"):
            for k in range(3):
                g_copy(k, w).wait_recv()
        g_sum[w] += g_recv[0, w].astype(F32) + g_recv[1, w].astype(F32) + g_recv[2, w].astype(F32)
        for d in (1, 2, 3):
            gz_send[w, d - 1] = g_sum[w, pl.ds(pl.multiple_of(u * lax.rem(zl + d, 4), u), u)].astype(BF)
            send(h_copy(w, d))

    steps = dict(
        z=w_take, w=w_relay, b=lambda n: (a_wait(n, 0), a_wait(n, 1)), c=near, e=near_out, p=p_send, q=p_pass, g=weight_part,
        n=onward, r=onward3, o=lambda n: offer(3, n), d=lambda n: deliver(3, n), y=over_y,
    )
    single = dict(ar=a_relay, ow=own_part, of=own_sum, a3=lambda: (a_wait(3, 0), a_wait(3, 1)))
    for step in PLAN:
        if step in single:
            single[step]()
        else:
            steps[step[0]](int(step[1]))

    with jax.named_scope("s21_cwait"):

        @pl.when(x != 2 * zh + cc)
        def _():
            for n in range(4):
                arrived(zh, n)

    with jax.named_scope("s22_zwait"):
        for n in range(4):
            across(n).wait_recv()
    for n in range(4):
        cols = w_cols(n)
        own_pre = pre[:, pl.ds(pl.multiple_of(q * (2 * zh + cc) + v * lax.rem(y + 4 - FROM[n], 4), v), v)]
        both = c_in[zh, n].astype(F32) + z_in[n].astype(F32)
        gout[:, cols] = jnp.where(own_pre.astype(F32) > 0, both, 0.0).astype(BF)

    for w in (0, 1):
        with jax.named_scope("s23_hwait"):
            for d in (1, 2, 3):
                h_copy(w, d).wait_recv()
        total = g_sum[w, pl.ds(pl.multiple_of(u * zl, u), u)]
        total += gz_recv[w, 0].astype(F32) + gz_recv[w, 1].astype(F32) + gz_recv[w, 2].astype(F32)
        wout[:, w * 2 * v:(w + 1) * 2 * v] = total * scale

    for c in sent:
        c.wait_send()
    for n in range(4):
        across(n).wait_send()

    @pl.when(cc != lead)
    def _():
        own.wait_send()


def store(w_v, g_v, w_h, g_h, sems):
    copies = [pltpu.make_async_copy(w_v, w_h, sems.at[0]), pltpu.make_async_copy(g_v, g_h, sems.at[1])]
    for c in copies:
        c.start()
    for c in copies:
        c.wait()


def per_device(pre_act, grad_out, w_down):
    t, q = grad_out.shape
    u = w_down.shape[0]
    v = 4 * u
    half = t // 2
    vm = pltpu.VMEM
    sem = lambda *n: pltpu.SemaphoreType.DMA(n)
    space = pl.BlockSpec(memory_space=pltpu.VMEM)
    hbm = pl.BlockSpec(memory_space=pltpu.HBM)
    outs = pl.pallas_call(
        body,
        out_shape=(pltpu.VMEM((u, q), F32), pltpu.VMEM((t, q), BF)),
        in_specs=[hbm] * 3,
        out_specs=(space, space),
        scratch_shapes=[
            vm((t, pre_act.shape[1]), BF),
            vm((4 * t, q), BF), vm((4, 4 * t, v), BF), vm((4 * v, q), BF), vm((v, 4 * t), BF),
            vm((t, v), F32), vm((4, t, v), F32), vm((4, t, v), BF), vm((4, t, v), BF),
            vm((3, 4, half, v), F32), vm((3, 4, half, v), BF), vm((3, 4, half, v), BF), vm((3, 4, half, v), BF),
            vm((2, 4, t, v), BF), vm((4, t, v), BF),
            vm((3, 2, v, q // 2), BF), vm((3, 2, v, q // 2), BF), vm((2, v, q // 2), F32),
            vm((2, 3, u, q // 2), BF), vm((2, 3, u, q // 2), BF),
            sem(3), sem(3), sem(3), sem(3, 4), sem(3, 4), sem(3, 2), sem(3, 2),
            sem(3, 4), sem(3, 4), sem(3, 4), sem(3, 4),
            sem(1), sem(1), sem(3, 4), sem(3, 4), sem(3, 4), sem(2, 4, 2),
            sem(4), sem(4), sem(3, 2), sem(3, 2), sem(2, 3), sem(2, 3),
        ],
        compiler_params=pltpu.CompilerParams(
            collective_id=0, has_side_effects=True, vmem_limit_bytes=62_400_000
        ),
        name="backward",
    )(pre_act, grad_out, w_down)
    return pl.pallas_call(
        store,
        out_shape=(jax.ShapeDtypeStruct((u, q), F32), jax.ShapeDtypeStruct((t, q), BF)),
        in_specs=[space] * 2,
        out_specs=(hbm, hbm),
        scratch_shapes=[sem(2)],
        compiler_params=pltpu.CompilerParams(vmem_limit_bytes=2**20),
        name="store",
    )(*outs)


def solution(mesh):
    torus = Mesh(mesh.devices.reshape(2, mesh.shape["row"] // 2, 4, 4, 4), AXES)
    return jax.shard_map(
        per_device,
        mesh=torus,
        in_specs=(P(COL, None), P(COL, ROW), P(COL, ROW)),
        out_specs=(P(COL, ROW), P(COL, ROW)),
        check_vma=False,
    )
```

```python
import jax
import jax.numpy as jnp
from jax import lax
from jax.experimental import pallas as pl
from jax.experimental.pallas import tpu as pltpu
from jax.sharding import Mesh
from jax.sharding import PartitionSpec as P

AXES = ("zh", "cc", "x", "y", "zl")
COL = ("x", "y", "zl")
ROW = ("zh", "cc")
MESH = pl.DeviceIdType.MESH
BF = jnp.bfloat16
F32 = jnp.float32
TURNS = (2, 1, 3, 0)
PLAN = (
    "p0", "z1", "w0", "z2", "w1", "z3", "b1", "b2", "c0", "w2", "w3", "c1",
    "e0", "c2", "e1", "ar", "c3", "e2", "e3", "p1", "ow", "n0", "n1", "of",
    "q0", "a3", "g0", "n2", "n3", "o0", "o1", "d0", "o2", "d1", "p2", "o3",
    "d2", "p3", "d3", "q1", "g1", "r0", "r1", "q2", "g2", "r2", "q3", "g3",
    "r3", "y0", "k0", "y1", "k1",
)
FROM = (0, 1, 3, 2)


def body(
    pre_h, go_h, wd_h, wout, gout,
    pre, a_all, p_all, w_all, pt, acc, o_keep, o_give, o_take, keep, c_give, c_take, c_send, c_in, z_in,
    g_send, g_recv, g_sum, gz_send, gz_recv, gz_pass,
    l_s, wz_s, wz_r, wy_s, wy_r, a_s, a_r, p_s, p_r, q_s, q_r, o_s, o_r, d_s, d_r, c_s, c_r,
    z_s, z_r, g_s, g_r, h_s, h_r, k_r,
):
    zh, cc, x, y, zl = [lax.axis_index(name) for name in AXES]
    t, q = go_h.shape
    half = t // 2
    u = wd_h.shape[0]
    v = 4 * u
    scale = 1.0 / jnp.sqrt(jnp.float32(t * 64))

    def dev(dx=0, dy=0, dz=0, core=None, other=False):
        return (
            1 - zh if other else zh,
            cc if core is None else core,
            lax.rem(x + dx, 4),
            lax.rem(y + dy, 4),
            lax.rem(zl + dz, 4),
        )

    def copy(src, dst, ss, rs, to):
        return pltpu.make_async_remote_copy(
            src_ref=src, dst_ref=dst, send_sem=ss, recv_sem=rs, device_id=to, device_id_type=MESH
        )

    def w_rows(yy, zz):
        return pl.ds(pl.multiple_of(v * yy + u * zz, u), u)

    def w_block(dy, d):
        return w_all.at[w_rows(lax.rem(y + 4 - dy, 4), lax.rem(zl + 4 - d, 4))]

    def p_cols(dx, k):
        block = q * lax.rem(x + dx, 4) + v * lax.rem(y + TURNS[k], 4)
        return pl.ds(pl.multiple_of(block, v), v)

    twin = 1 - cc
    lead = lax.rem(x, 2)
    peers = [dev(core=twin), dev(other=True)]
    peers += [dev(dx=d, core=c) for d in (1, 2, 3) for c in (cc, twin)]
    peers += [dev(dy=d) for d in (1, 2, 3)] + [dev(dz=d) for d in (1, 2, 3)]
    with jax.named_scope("s00_barrier"):
        barrier = pltpu.get_barrier_semaphore()
        for peer in peers:
            pl.semaphore_signal(barrier, inc=1, device_id=peer, device_id_type=MESH)

    load_w = pltpu.make_async_copy(wd_h, w_block(0, 0), l_s.at[0])
    load_a = pltpu.make_async_copy(go_h, a_all.at[0:t], l_s.at[1])
    load_p = pltpu.make_async_copy(pre_h, pre, l_s.at[2])
    loads = [load_w, load_a, load_p]
    for c in loads:
        c.start()
    with jax.named_scope("s01_loads"):
        load_w.wait()
        load_a.wait()
    with jax.named_scope("s02_barrier"):
        pl.semaphore_wait(barrier, len(peers))

    sent = []

    def send(c):
        c.start()
        sent.append(c)

    def wz(d):
        return copy(w_block(0, 0), w_block(0, 0), wz_s.at[d - 1], wz_r.at[d - 1], dev(dz=d))

    def wy(e, d):
        block = (w_block(0, d), w_block(0, d), w_block(1, d) if d % 2 == 0 else w_block(3, d))[e]
        dy = (1, 3, 1 if d % 2 == 0 else 3)[e]
        return copy(block, block, wy_s.at[e, d], wy_r.at[e, d], dev(dy=dy))

    def wy_wait(e, d):
        block = w_block((1, 3, 2)[e], d)
        copy(block, block, wy_s.at[e, d], wy_r.at[e, d], dev(dy=1)).wait_recv()

    def a_half(slot, h):
        return a_all.at[pl.ds(t * slot + half * h, half)]

    for d in (1, 2, 3):
        send(wz(d))
    send(wy(0, 0))
    send(wy(1, 0))
    for h in (0, 1):
        send(copy(a_half(0, h), a_half(1, h), a_s.at[0, h], a_r.at[0, h], dev(dx=1)))
        g = 1 - h
        send(copy(a_half(0, g), a_half(2, g), a_s.at[1, g], a_r.at[1, g], dev(dx=3)))

    mine = pl.ds(pl.multiple_of(half * cc, half), half)
    theirs = pl.ds(pl.multiple_of(half * twin, half), half)

    def p_copy(slot, k):
        dx = (1, 3, 2)[slot - 1]
        rows = pl.ds(pl.multiple_of(t * slot + half * cc, half), half)
        return copy(
            pre.at[mine, p_cols(dx, k)], p_all.at[k, rows], p_s.at[slot - 1, k], p_r.at[slot - 1, k], dev(dx=dx)
        )

    def q_copy(slot, k):
        rows = p_all.at[k, pl.ds(pl.multiple_of(t * slot + half * cc, half), half)]
        return copy(rows, rows, q_s.at[slot - 1, k], q_r.at[slot - 1, k], dev(core=twin))

    def p_send(k):
        for slot in (1, 2, 3):
            send(p_copy(slot, k))

    load_p.wait()

    with jax.named_scope("s03_local"):
        for k in range(4):
            p_all[k, 0:t] = pre[:, p_cols(0, k)]

    def a_wait(slot, h):
        copy(a_half(slot, h), a_half(slot, h), a_s.at[slot - 1, h], a_r.at[slot - 1, h], dev(dx=1)).wait_recv()

    def a_relay():
        send(copy(a_half(1, 0), a_half(3, 0), a_s.at[2, 0], a_r.at[2, 0], dev(dx=1)))
        send(copy(a_half(2, 1), a_half(3, 1), a_s.at[2, 1], a_r.at[2, 1], dev(dx=3)))

    def w_relay(d):
        with jax.named_scope("s05_wy"):
            wy_wait(d % 2, d)
            send(wy(2, d))

    def w_take(d):
        with jax.named_scope("s04_wz"):
            block = w_block(0, d)
            copy(block, block, wz_s.at[d - 1], wz_r.at[d - 1], dev(dz=d)).wait_recv()
            send(wy(0, d))
            send(wy(1, d))

    def w_cols(n):
        return pl.ds(pl.multiple_of(v * lax.rem(y + 4 - FROM[n], 4), v), v)

    def partial(slot, n, out):
        out[...] = lax.dot_general(
            a_all[t * slot:t * slot + t], w_all[w_cols(n), :], (((1,), (1,)), ((), ())),
            preferred_element_type=F32,
        )

    def swap(slot, n):
        i = slot - 1
        return copy(c_give.at[i, n], c_take.at[i, n], d_s.at[i, n], d_r.at[i, n], dev(core=twin))

    def offer(slot, n):
        partial(slot, n, acc)
        c_give[slot - 1, n] = acc[theirs].astype(BF)
        keep[slot - 1, n] = acc[mine]
        send(swap(slot, n))

    def deliver(slot, n):
        i = slot - 1
        swap(slot, n).wait_recv()
        c_send[i, n] = (keep[i, n] + c_take[i, n].astype(F32)).astype(BF)
        target = c_in.at[lax.div(x, 2), n, mine]
        to = dev(dx=(3, 1, 2)[i], core=lead)
        send(copy(c_send.at[i, n], target, c_s.at[i, n], c_r.at[lax.div(x, 2), n, cc], to))

    def arrived(i, n):
        for h in (0, 1):
            rows = c_in.at[i, n, pl.ds(half * h, half)]
            copy(rows, rows, c_s.at[0, 0], c_r.at[i, n, h], dev(dx=1)).wait_recv()

    def across(n):
        return copy(c_in.at[1 - zh, n], z_in.at[n], z_s.at[n], z_r.at[n], dev(other=True))

    far = lax.rem(2 * (1 - zh) + cc + 4 - x, 4)

    def onward(n):
        with jax.named_scope("s10_onward1"):

            @pl.when((far == 1) | (far == 3))
            def _():
                arrived(1 - zh, n)
                across(n).start()

    def near(n):
        with jax.named_scope("s07_wy"):
            if n in (1, 2):
                for d in range(4):
                    if d % 2 == n % 2:
                        wy_wait(n - 1, d)
            if n == 3:
                for d in range(4):
                    wy_wait(2, d)
        with jax.named_scope("s08_offer12"):
            offer(1, n)
            offer(2, n)

    def near_out(n):
        with jax.named_scope("s08_deliver12"):
            deliver(1, n)
            deliver(2, n)

    own = copy(o_give, o_take, o_s.at[0], o_r.at[0], dev(core=twin))

    def own_part():
        with jax.named_scope("s09_own"):
            for n in range(4):
                partial(0, n, o_keep.at[n])

            @pl.when(cc != lead)
            def _():
                o_give[...] = o_keep[...].astype(BF)
                own.start()

    def own_sum():
        with jax.named_scope("s11_own"):

            @pl.when(cc == lead)
            def _():
                own.wait_recv()
                c_in[lax.div(x, 2)] = (o_keep[...] + o_take[...].astype(F32)).astype(BF)

                @pl.when(far == 0)
                def _():
                    for n in range(4):
                        across(n).start()

    def p_pass(k):
        with jax.named_scope("s14_pwait"):
            for slot in (1, 2, 3):
                p_copy(slot, k).wait_recv()
                send(q_copy(slot, k))

    def g_copy(k, w):
        return copy(g_send.at[k, w], g_recv.at[k, w], g_s.at[k, w], g_r.at[k, w], dev(dy=TURNS[k]))

    def weight_part(k):
        with jax.named_scope("s15_qwait"):
            for slot in (1, 2, 3):
                q_copy(slot, k).wait_recv()
        with jax.named_scope("s16_g"):
            pt[...] = jnp.maximum(p_all[k], jnp.zeros((), BF)).T

            for w in (0, 1):

                @pl.loop(0, 2)
                def _(n):
                    cols = pl.ds(pl.multiple_of(n * v, v), v)
                    from_cols = pl.ds(pl.multiple_of((2 * w + n) * v, v), v)
                    part = jnp.dot(pt[...], a_all[:, from_cols], preferred_element_type=F32)
                    if k < 3:
                        g_send[k, w, :, cols] = part.astype(BF)
                    else:
                        g_sum[w, :, cols] = part

                if k < 3:
                    send(g_copy(k, w))

    def onward3(n):
        with jax.named_scope("s17_onward3"):

            @pl.when(far == 2)
            def _():
                arrived(1 - zh, n)
                across(n).start()

    at_end = (zl == 0) | (zl == 3)
    inner = lax.div(zl, 3) + 1
    end = 3 * (zl - 1)

    def z_start(w, j, block, to, target, recv, more=None):
        total = g_sum[w, pl.ds(pl.multiple_of(u * block, u), u)]
        if more is not None:
            total += more[...].astype(F32)
        gz_send[w, j] = total.astype(BF)
        copy(gz_send.at[w, j], target, h_s.at[w, j], recv, (zh, cc, x, y, to)).start()

    def over_y(w):
        with jax.named_scope("s20_gwait"):
            for k in range(3):
                g_copy(k, w).wait_recv()
        g_sum[w] += g_recv[0, w].astype(F32) + g_recv[1, w].astype(F32) + g_recv[2, w].astype(F32)

        @pl.when(at_end)
        def _():
            z_start(w, 0, 3 - zl, inner, gz_pass.at[w], k_r.at[w])
            z_start(w, 2, 3 - inner, 3 - inner, gz_recv.at[w, 2], h_r.at[w, 2])
            z_start(w, 1, inner, inner, gz_recv.at[w, 0], h_r.at[w, 0])

        @pl.when(jnp.logical_not(at_end))
        def _():
            z_start(w, 0, 3 - zl, 3 - zl, gz_recv.at[w, 1], h_r.at[w, 1])
            z_start(w, 1, end, end, gz_recv.at[w, 0], h_r.at[w, 0])

    def z_wait(w, j):
        copy(gz_send.at[w, j], gz_recv.at[w, j], h_s.at[w, j], h_r.at[w, j], dev(dz=1)).wait_recv()

    def pass_on(w):
        with jax.named_scope("s21_pass"):

            @pl.when(jnp.logical_not(at_end))
            def _():
                copy(gz_send.at[w, 2], gz_pass.at[w], h_s.at[w, 2], k_r.at[w], dev(dz=1)).wait_recv()
                z_start(w, 2, 3 - end, 3 - end, gz_recv.at[w, 1], h_r.at[w, 1], gz_pass.at[w])

    steps = dict(
        z=w_take, w=w_relay, b=lambda n: (a_wait(n, 0), a_wait(n, 1)), c=near, e=near_out, p=p_send, q=p_pass, g=weight_part,
        n=onward, r=onward3, o=lambda n: offer(3, n), d=lambda n: deliver(3, n), y=over_y, k=pass_on,
    )
    single = dict(ar=a_relay, ow=own_part, of=own_sum, a3=lambda: (a_wait(3, 0), a_wait(3, 1)))
    for step in PLAN:
        if step in single:
            single[step]()
        else:
            steps[step[0]](int(step[1]))

    with jax.named_scope("s21_cwait"):

        @pl.when(x != 2 * zh + cc)
        def _():
            for n in range(4):
                arrived(zh, n)

    with jax.named_scope("s22_zwait"):
        for n in range(4):
            across(n).wait_recv()
    for n in range(4):
        cols = w_cols(n)
        own_pre = pre[:, pl.ds(pl.multiple_of(q * (2 * zh + cc) + v * lax.rem(y + 4 - FROM[n], 4), v), v)]
        both = c_in[zh, n].astype(F32) + z_in[n].astype(F32)
        gout[:, cols] = jnp.where(own_pre.astype(F32) > 0, both, 0.0).astype(BF)

    for w in (0, 1):
        with jax.named_scope("s23_hwait"):
            for j in (0, 1):
                z_wait(w, j)

        cols = pl.ds(w * 2 * v, 2 * v)
        total = g_sum[w, pl.ds(pl.multiple_of(u * zl, u), u)]
        total += gz_recv[w, 0].astype(F32) + gz_recv[w, 1].astype(F32)

        @pl.when(at_end)
        def _():
            wout[:, cols] = total * scale

        @pl.when(jnp.logical_not(at_end))
        def _():
            z_wait(w, 2)
            wout[:, cols] = (total + gz_recv[w, 2].astype(F32)) * scale

    for c in sent:
        c.wait_send()
    for n in range(4):
        across(n).wait_send()
    for w in (0, 1):
        for j in range(3):
            copy(gz_send.at[w, j], gz_recv.at[w, j], h_s.at[w, j], h_r.at[w, j], dev(dz=1)).wait_send()

    @pl.when(cc != lead)
    def _():
        own.wait_send()


def store(w_v, g_v, w_h, g_h, sems):
    copies = [pltpu.make_async_copy(w_v, w_h, sems.at[0]), pltpu.make_async_copy(g_v, g_h, sems.at[1])]
    for c in copies:
        c.start()
    for c in copies:
        c.wait()


def per_device(pre_act, grad_out, w_down):
    t, q = grad_out.shape
    u = w_down.shape[0]
    v = 4 * u
    half = t // 2
    vm = pltpu.VMEM
    sem = lambda *n: pltpu.SemaphoreType.DMA(n)
    space = pl.BlockSpec(memory_space=pltpu.VMEM)
    hbm = pl.BlockSpec(memory_space=pltpu.HBM)
    outs = pl.pallas_call(
        body,
        out_shape=(pltpu.VMEM((u, q), F32), pltpu.VMEM((t, q), BF)),
        in_specs=[hbm] * 3,
        out_specs=(space, space),
        scratch_shapes=[
            vm((t, pre_act.shape[1]), BF),
            vm((4 * t, q), BF), vm((4, 4 * t, v), BF), vm((4 * v, q), BF), vm((v, 4 * t), BF),
            vm((t, v), F32), vm((4, t, v), F32), vm((4, t, v), BF), vm((4, t, v), BF),
            vm((3, 4, half, v), F32), vm((3, 4, half, v), BF), vm((3, 4, half, v), BF), vm((3, 4, half, v), BF),
            vm((2, 4, t, v), BF), vm((4, t, v), BF),
            vm((3, 2, v, q // 2), BF), vm((3, 2, v, q // 2), BF), vm((2, v, q // 2), F32),
            vm((2, 3, u, q // 2), BF), vm((2, 3, u, q // 2), BF), vm((2, u, q // 2), BF),
            sem(3), sem(3), sem(3), sem(3, 4), sem(3, 4), sem(3, 2), sem(3, 2),
            sem(3, 4), sem(3, 4), sem(3, 4), sem(3, 4),
            sem(1), sem(1), sem(3, 4), sem(3, 4), sem(3, 4), sem(2, 4, 2),
            sem(4), sem(4), sem(3, 2), sem(3, 2), sem(2, 3), sem(2, 3), sem(2),
        ],
        compiler_params=pltpu.CompilerParams(
            collective_id=0, has_side_effects=True, vmem_limit_bytes=62_400_000
        ),
        name="backward",
    )(pre_act, grad_out, w_down)
    return pl.pallas_call(
        store,
        out_shape=(jax.ShapeDtypeStruct((u, q), F32), jax.ShapeDtypeStruct((t, q), BF)),
        in_specs=[space] * 2,
        out_specs=(hbm, hbm),
        scratch_shapes=[sem(2)],
        compiler_params=pltpu.CompilerParams(vmem_limit_bytes=2**20),
        name="store",
    )(*outs)


def solution(mesh):
    torus = Mesh(mesh.devices.reshape(2, mesh.shape["row"] // 2, 4, 4, 4), AXES)
    return jax.shard_map(
        per_device,
        mesh=torus,
        in_specs=(P(COL, None), P(COL, ROW), P(COL, ROW)),
        out_specs=(P(COL, ROW), P(COL, ROW)),
        check_vma=False,
    )
```

```python
import jax
import jax.numpy as jnp
from jax import lax
from jax.experimental import pallas as pl
from jax.experimental.pallas import tpu as pltpu
from jax.sharding import Mesh
from jax.sharding import PartitionSpec as P

AXES = ("zh", "cc", "x", "y", "zl")
COL = ("x", "y", "zl")
ROW = ("zh", "cc")
MESH = pl.DeviceIdType.MESH
BF = jnp.bfloat16
F32 = jnp.float32
TURNS = (2, 1, 3, 0)
PLAN = (
    "p0", "z1", "w0", "z2", "w1", "z3", "b1", "b2", "c0", "w2", "w3", "c1",
    "e0", "c2", "e1", "ar", "c3", "e2", "e3", "p1", "ow", "n0", "n1", "of",
    "q0", "a3", "g0", "n2", "n3", "o0", "o1", "d0", "d1", "p2", "o2", "o3",
    "d2", "d3", "p3", "q1", "g1", "r0", "r1", "q2", "g2", "r2", "r3", "q3",
    "g3", "y0", "k0", "y1", "k1",
)
FROM = (0, 1, 3, 2)


def body(
    pre_h, go_h, wd_h, wout, gout,
    pre, a_all, p_all, w_all, pt, acc, o_keep, o_give, o_take, keep, c_give, c_take, c_send, c_in, z_in,
    g_send, g_recv, g_sum, gz_send, gz_recv, gz_pass,
    l_s, wz_s, wz_r, wy_s, wy_r, a_s, a_r, p_s, p_r, q_s, q_r, o_s, o_r, d_s, d_r, c_s, c_r,
    z_s, z_r, g_s, g_r, h_s, h_r, k_r,
):
    zh, cc, x, y, zl = [lax.axis_index(name) for name in AXES]
    t, q = go_h.shape
    half = t // 2
    u = wd_h.shape[0]
    v = 4 * u
    scale = 1.0 / jnp.sqrt(jnp.float32(t * 64))

    def dev(dx=0, dy=0, dz=0, core=None, other=False):
        return (
            1 - zh if other else zh,
            cc if core is None else core,
            lax.rem(x + dx, 4),
            lax.rem(y + dy, 4),
            lax.rem(zl + dz, 4),
        )

    def copy(src, dst, ss, rs, to):
        return pltpu.make_async_remote_copy(
            src_ref=src, dst_ref=dst, send_sem=ss, recv_sem=rs, device_id=to, device_id_type=MESH
        )

    def w_rows(yy, zz):
        return pl.ds(pl.multiple_of(v * yy + u * zz, u), u)

    def w_block(dy, d):
        return w_all.at[w_rows(lax.rem(y + 4 - dy, 4), lax.rem(zl + 4 - d, 4))]

    def p_cols(dx, k):
        block = q * lax.rem(x + dx, 4) + v * lax.rem(y + TURNS[k], 4)
        return pl.ds(pl.multiple_of(block, v), v)

    twin = 1 - cc
    lead = lax.rem(x, 2)
    peers = [dev(core=twin), dev(other=True)]
    peers += [dev(dx=d, core=c) for d in (1, 2, 3) for c in (cc, twin)]
    peers += [dev(dy=d) for d in (1, 2, 3)] + [dev(dz=d) for d in (1, 2, 3)]
    with jax.named_scope("s00_barrier"):
        barrier = pltpu.get_barrier_semaphore()
        for peer in peers:
            pl.semaphore_signal(barrier, inc=1, device_id=peer, device_id_type=MESH)

    load_w = pltpu.make_async_copy(wd_h, w_block(0, 0), l_s.at[0])
    load_a = pltpu.make_async_copy(go_h, a_all.at[0:t], l_s.at[1])
    load_p = pltpu.make_async_copy(pre_h, pre, l_s.at[2])
    loads = [load_w, load_a, load_p]
    for c in loads:
        c.start()
    with jax.named_scope("s01_loads"):
        load_w.wait()
        load_a.wait()
    with jax.named_scope("s02_barrier"):
        pl.semaphore_wait(barrier, len(peers))

    sent = []

    def send(c):
        c.start()
        sent.append(c)

    def wz(d):
        return copy(w_block(0, 0), w_block(0, 0), wz_s.at[d - 1], wz_r.at[d - 1], dev(dz=d))

    def wy(e, d):
        block = (w_block(0, d), w_block(0, d), w_block(1, d) if d % 2 == 0 else w_block(3, d))[e]
        dy = (1, 3, 1 if d % 2 == 0 else 3)[e]
        return copy(block, block, wy_s.at[e, d], wy_r.at[e, d], dev(dy=dy))

    def wy_wait(e, d):
        block = w_block((1, 3, 2)[e], d)
        copy(block, block, wy_s.at[e, d], wy_r.at[e, d], dev(dy=1)).wait_recv()

    def a_half(slot, h):
        return a_all.at[pl.ds(t * slot + half * h, half)]

    for d in (1, 2, 3):
        send(wz(d))
    send(wy(0, 0))
    send(wy(1, 0))
    for h in (0, 1):
        send(copy(a_half(0, h), a_half(1, h), a_s.at[0, h], a_r.at[0, h], dev(dx=1)))
        g = 1 - h
        send(copy(a_half(0, g), a_half(2, g), a_s.at[1, g], a_r.at[1, g], dev(dx=3)))

    mine = pl.ds(pl.multiple_of(half * cc, half), half)
    theirs = pl.ds(pl.multiple_of(half * twin, half), half)

    def p_copy(slot, k):
        dx = (1, 3, 2)[slot - 1]
        rows = pl.ds(pl.multiple_of(t * slot + half * cc, half), half)
        return copy(
            pre.at[mine, p_cols(dx, k)], p_all.at[k, rows], p_s.at[slot - 1, k], p_r.at[slot - 1, k], dev(dx=dx)
        )

    def q_copy(slot, k):
        rows = p_all.at[k, pl.ds(pl.multiple_of(t * slot + half * cc, half), half)]
        return copy(rows, rows, q_s.at[slot - 1, k], q_r.at[slot - 1, k], dev(core=twin))

    def p_send(k):
        for slot in (1, 2, 3):
            send(p_copy(slot, k))

    load_p.wait()

    with jax.named_scope("s03_local"):
        for k in range(4):
            p_all[k, 0:t] = pre[:, p_cols(0, k)]

    def a_wait(slot, h):
        copy(a_half(slot, h), a_half(slot, h), a_s.at[slot - 1, h], a_r.at[slot - 1, h], dev(dx=1)).wait_recv()

    def a_relay():
        send(copy(a_half(1, 0), a_half(3, 0), a_s.at[2, 0], a_r.at[2, 0], dev(dx=1)))
        send(copy(a_half(2, 1), a_half(3, 1), a_s.at[2, 1], a_r.at[2, 1], dev(dx=3)))

    def w_relay(d):
        with jax.named_scope("s05_wy"):
            wy_wait(d % 2, d)
            send(wy(2, d))

    def w_take(d):
        with jax.named_scope("s04_wz"):
            block = w_block(0, d)
            copy(block, block, wz_s.at[d - 1], wz_r.at[d - 1], dev(dz=d)).wait_recv()
            send(wy(0, d))
            send(wy(1, d))

    def w_cols(n):
        return pl.ds(pl.multiple_of(v * lax.rem(y + 4 - FROM[n], 4), v), v)

    def partial(slot, n, out):
        out[...] = lax.dot_general(
            a_all[t * slot:t * slot + t], w_all[w_cols(n), :], (((1,), (1,)), ((), ())),
            preferred_element_type=F32,
        )

    def swap(slot, n):
        i = slot - 1
        return copy(c_give.at[i, n], c_take.at[i, n], d_s.at[i, n], d_r.at[i, n], dev(core=twin))

    def offer(slot, n):
        partial(slot, n, acc)
        c_give[slot - 1, n] = acc[theirs].astype(BF)
        keep[slot - 1, n] = acc[mine]
        send(swap(slot, n))

    def deliver(slot, n):
        i = slot - 1
        swap(slot, n).wait_recv()
        c_send[i, n] = (keep[i, n] + c_take[i, n].astype(F32)).astype(BF)
        target = c_in.at[lax.div(x, 2), n, mine]
        to = dev(dx=(3, 1, 2)[i], core=lead)
        send(copy(c_send.at[i, n], target, c_s.at[i, n], c_r.at[lax.div(x, 2), n, cc], to))

    def arrived(i, n):
        for h in (0, 1):
            rows = c_in.at[i, n, pl.ds(half * h, half)]
            copy(rows, rows, c_s.at[0, 0], c_r.at[i, n, h], dev(dx=1)).wait_recv()

    def across(n):
        return copy(c_in.at[1 - zh, n], z_in.at[n], z_s.at[n], z_r.at[n], dev(other=True))

    far = lax.rem(2 * (1 - zh) + cc + 4 - x, 4)

    def onward(n):
        with jax.named_scope("s10_onward1"):

            @pl.when((far == 1) | (far == 3))
            def _():
                arrived(1 - zh, n)
                across(n).start()

    def near(n):
        with jax.named_scope("s07_wy"):
            if n in (1, 2):
                for d in range(4):
                    if d % 2 == n % 2:
                        wy_wait(n - 1, d)
            if n == 3:
                for d in range(4):
                    wy_wait(2, d)
        with jax.named_scope("s08_offer12"):
            offer(1, n)
            offer(2, n)

    def near_out(n):
        with jax.named_scope("s08_deliver12"):
            deliver(1, n)
            deliver(2, n)

    own = copy(o_give, o_take, o_s.at[0], o_r.at[0], dev(core=twin))

    def own_part():
        with jax.named_scope("s09_own"):
            for n in range(4):
                partial(0, n, o_keep.at[n])

            @pl.when(cc != lead)
            def _():
                o_give[...] = o_keep[...].astype(BF)
                own.start()

    def own_sum():
        with jax.named_scope("s11_own"):

            @pl.when(cc == lead)
            def _():
                own.wait_recv()
                c_in[lax.div(x, 2)] = (o_keep[...] + o_take[...].astype(F32)).astype(BF)

                @pl.when(far == 0)
                def _():
                    for n in range(4):
                        across(n).start()

    def p_pass(k):
        with jax.named_scope("s14_pwait"):
            for slot in (1, 2, 3):
                p_copy(slot, k).wait_recv()
                send(q_copy(slot, k))

    def g_copy(k, w):
        return copy(g_send.at[k, w], g_recv.at[k, w], g_s.at[k, w], g_r.at[k, w], dev(dy=TURNS[k]))

    def weight_part(k):
        with jax.named_scope("s15_qwait"):
            for slot in (1, 2, 3):
                q_copy(slot, k).wait_recv()
        with jax.named_scope("s16_g"):
            pt[...] = jnp.maximum(p_all[k], jnp.zeros((), BF)).T

            for w in (0, 1):

                @pl.loop(0, 2)
                def _(n):
                    cols = pl.ds(pl.multiple_of(n * v, v), v)
                    from_cols = pl.ds(pl.multiple_of((2 * w + n) * v, v), v)
                    part = jnp.dot(pt[...], a_all[:, from_cols], preferred_element_type=F32)
                    if k < 3:
                        g_send[k, w, :, cols] = part.astype(BF)
                    else:
                        g_sum[w, :, cols] = part

                if k < 3:
                    send(g_copy(k, w))

    def onward3(n):
        with jax.named_scope("s17_onward3"):

            @pl.when(far == 2)
            def _():
                arrived(1 - zh, n)
                across(n).start()

    at_end = (zl == 0) | (zl == 3)
    inner = lax.div(zl, 3) + 1
    end = 3 * (zl - 1)

    def z_start(w, j, block, to, target, recv, more=None):
        total = g_sum[w, pl.ds(pl.multiple_of(u * block, u), u)]
        if more is not None:
            total += more[...].astype(F32)
        gz_send[w, j] = total.astype(BF)
        copy(gz_send.at[w, j], target, h_s.at[w, j], recv, (zh, cc, x, y, to)).start()

    def over_y(w):
        with jax.named_scope("s20_gwait"):
            for k in range(3):
                g_copy(k, w).wait_recv()
        g_sum[w] += g_recv[0, w].astype(F32) + g_recv[1, w].astype(F32) + g_recv[2, w].astype(F32)

        @pl.when(at_end)
        def _():
            z_start(w, 0, 3 - zl, inner, gz_pass.at[w], k_r.at[w])
            z_start(w, 2, 3 - inner, 3 - inner, gz_recv.at[w, 2], h_r.at[w, 2])
            z_start(w, 1, inner, inner, gz_recv.at[w, 0], h_r.at[w, 0])

        @pl.when(jnp.logical_not(at_end))
        def _():
            z_start(w, 0, 3 - zl, 3 - zl, gz_recv.at[w, 1], h_r.at[w, 1])
            z_start(w, 1, end, end, gz_recv.at[w, 0], h_r.at[w, 0])

    def z_wait(w, j):
        copy(gz_send.at[w, j], gz_recv.at[w, j], h_s.at[w, j], h_r.at[w, j], dev(dz=1)).wait_recv()

    def pass_on(w):
        with jax.named_scope("s21_pass"):

            @pl.when(jnp.logical_not(at_end))
            def _():
                copy(gz_send.at[w, 2], gz_pass.at[w], h_s.at[w, 2], k_r.at[w], dev(dz=1)).wait_recv()
                z_start(w, 2, 3 - end, 3 - end, gz_recv.at[w, 1], h_r.at[w, 1], gz_pass.at[w])

    steps = dict(
        z=w_take, w=w_relay, b=lambda n: (a_wait(n, 0), a_wait(n, 1)), c=near, e=near_out, p=p_send, q=p_pass, g=weight_part,
        n=onward, r=onward3, o=lambda n: offer(3, n), d=lambda n: deliver(3, n), y=over_y, k=pass_on,
    )
    single = dict(ar=a_relay, ow=own_part, of=own_sum, a3=lambda: (a_wait(3, 0), a_wait(3, 1)))
    for step in PLAN:
        if step in single:
            single[step]()
        else:
            steps[step[0]](int(step[1]))

    with jax.named_scope("s21_cwait"):

        @pl.when(x != 2 * zh + cc)
        def _():
            for n in range(4):
                arrived(zh, n)

    with jax.named_scope("s22_zwait"):
        for n in range(4):
            across(n).wait_recv()
    for n in range(4):
        cols = w_cols(n)
        own_pre = pre[:, pl.ds(pl.multiple_of(q * (2 * zh + cc) + v * lax.rem(y + 4 - FROM[n], 4), v), v)]
        both = c_in[zh, n].astype(F32) + z_in[n].astype(F32)
        gout[:, cols] = jnp.where(own_pre.astype(F32) > 0, both, 0.0).astype(BF)

    for w in (0, 1):
        with jax.named_scope("s23_hwait"):
            for j in (0, 1):
                z_wait(w, j)

        cols = pl.ds(w * 2 * v, 2 * v)
        total = g_sum[w, pl.ds(pl.multiple_of(u * zl, u), u)]
        total += gz_recv[w, 0].astype(F32) + gz_recv[w, 1].astype(F32)

        @pl.when(at_end)
        def _():
            wout[:, cols] = total * scale

        @pl.when(jnp.logical_not(at_end))
        def _():
            z_wait(w, 2)
            wout[:, cols] = (total + gz_recv[w, 2].astype(F32)) * scale

    for c in sent:
        c.wait_send()
    for n in range(4):
        across(n).wait_send()
    for w in (0, 1):
        for j in range(3):
            copy(gz_send.at[w, j], gz_recv.at[w, j], h_s.at[w, j], h_r.at[w, j], dev(dz=1)).wait_send()

    @pl.when(cc != lead)
    def _():
        own.wait_send()


def store(w_v, g_v, w_h, g_h, sems):
    copies = [pltpu.make_async_copy(w_v, w_h, sems.at[0]), pltpu.make_async_copy(g_v, g_h, sems.at[1])]
    for c in copies:
        c.start()
    for c in copies:
        c.wait()


def per_device(pre_act, grad_out, w_down):
    t, q = grad_out.shape
    u = w_down.shape[0]
    v = 4 * u
    half = t // 2
    vm = pltpu.VMEM
    sem = lambda *n: pltpu.SemaphoreType.DMA(n)
    space = pl.BlockSpec(memory_space=pltpu.VMEM)
    hbm = pl.BlockSpec(memory_space=pltpu.HBM)
    outs = pl.pallas_call(
        body,
        out_shape=(pltpu.VMEM((u, q), F32), pltpu.VMEM((t, q), BF)),
        in_specs=[hbm] * 3,
        out_specs=(space, space),
        scratch_shapes=[
            vm((t, pre_act.shape[1]), BF),
            vm((4 * t, q), BF), vm((4, 4 * t, v), BF), vm((4 * v, q), BF), vm((v, 4 * t), BF),
            vm((t, v), F32), vm((4, t, v), F32), vm((4, t, v), BF), vm((4, t, v), BF),
            vm((3, 4, half, v), F32), vm((3, 4, half, v), BF), vm((3, 4, half, v), BF), vm((3, 4, half, v), BF),
            vm((2, 4, t, v), BF), vm((4, t, v), BF),
            vm((3, 2, v, q // 2), BF), vm((3, 2, v, q // 2), BF), vm((2, v, q // 2), F32),
            vm((2, 3, u, q // 2), BF), vm((2, 3, u, q // 2), BF), vm((2, u, q // 2), BF),
            sem(3), sem(3), sem(3), sem(3, 4), sem(3, 4), sem(3, 2), sem(3, 2),
            sem(3, 4), sem(3, 4), sem(3, 4), sem(3, 4),
            sem(1), sem(1), sem(3, 4), sem(3, 4), sem(3, 4), sem(2, 4, 2),
            sem(4), sem(4), sem(3, 2), sem(3, 2), sem(2, 3), sem(2, 3), sem(2),
        ],
        compiler_params=pltpu.CompilerParams(
            collective_id=0, has_side_effects=True, vmem_limit_bytes=62_400_000
        ),
        name="backward",
    )(pre_act, grad_out, w_down)
    return pl.pallas_call(
        store,
        out_shape=(jax.ShapeDtypeStruct((u, q), F32), jax.ShapeDtypeStruct((t, q), BF)),
        in_specs=[space] * 2,
        out_specs=(hbm, hbm),
        scratch_shapes=[sem(2)],
        compiler_params=pltpu.CompilerParams(vmem_limit_bytes=2**20),
        name="store",
    )(*outs)


def solution(mesh):
    torus = Mesh(mesh.devices.reshape(2, mesh.shape["row"] // 2, 4, 4, 4), AXES)
    return jax.shard_map(
        per_device,
        mesh=torus,
        in_specs=(P(COL, None), P(COL, ROW), P(COL, ROW)),
        out_specs=(P(COL, ROW), P(COL, ROW)),
        check_vma=False,
    )
```
